32 devices in a mesh: grp: 4 (over y, x), chan: 8 (over z, core).
Axes of the slice: x: 2, y: 2, z: 4, core: 2. Of those that a mesh axis runs over, the one named last changes fastest.
Arguments:
- visibilities: float32 [4, 2, 8, 16, 2, 2048], P('grp', None, 'chan'), may hold values from -12 to 12
- model: bfloat16 [4, 2, 8, 8, 16, 2, 2048], P('grp', None, None, 'chan'), may hold values from -6 to 6
- flags: int32 [4, 8, 16, 2, 2048], P('grp', 'chan'), may hold values 0 or 1
- antennas: int32 [4, 2, 2048], P('grp'), may hold values from 0 to 63, as said below
- correlation: int32 [4, 4, 40], replicated, may hold values from -1 to 63, as said below
- gains_init: float32 [4, 2, 8, 8, 16, 64], P('grp', None, None, 'chan'), may hold values from -4 to 4
Outputs:
- final_jones_matrices: float32 [4, 2, 8, 8, 16, 64], P('grp', None, None, 'chan')
- consensus: float32 [4, 2, 8, 8, 16, 64], P('grp', None, None, 'chan')
- residual_vis: float32 [4, 2, 8, 16, 2, 2048], P('grp', None, 'chan')
The draws below stay inside these ranges and needn't reach their ends.
Inputs may be any that keep to these rules, and one draw needn't show every extreme that they name: antennas[g, 0, b] and antennas[g, 1, b] are different slots. correlation[g, h, j] and correlation[h, g, j] are the slots in clusters g and h of one shared station, or both -1; the live entries of a list are a prefix of it and distinct; correlation[g, g] is all -1; each pair of clusters shares 40 // 2 to 40 stations, and some pair exactly 40.
All inputs are finite; a program needn't handle non-finite values. No bound on the sum of `flags` on one device may be relied on, other than what follows from the above.
Results may differ from the reference program's by a relative error of at most 0.0003.
Values sent between devices are 32-bit elements; how exact they have to be, the bound alone decides.
A program may use at most 64 MiB of HBM per device.

```python
import jax
import jax.numpy as jnp
from jax import lax

K = 8
ST = 64
SHARED = 40
BL = 2048
SI = 16
TS = 2
ITERS = 2
CLUSTERS = 4
CHANNELS = 8


def draw_antennas(key, part):
    key_one, key_two = jax.random.split(jax.random.fold_in(key, 11))
    first = jax.random.randint(key_one, (CLUSTERS, BL), 0, ST)
    offset = jax.random.randint(key_two, (CLUSTERS, BL), 1, ST)
    second = (first + offset) % ST
    return jnp.stack([first, second], axis=1).astype(jnp.int32)


def draw_correlation(key, part):
    table = -jnp.ones((CLUSTERS, CLUSTERS, SHARED), jnp.int32)
    for cluster_index in range(CLUSTERS):
        for other in range(cluster_index + 1, CLUSTERS):
            subkey = jax.random.fold_in(key, 100 + cluster_index * CLUSTERS + other)
            key_one, key_two, key_three = jax.random.split(subkey, 3)
            live = jax.random.randint(key_three, (), SHARED // 2, SHARED + 1)
            if cluster_index == 0 and other == 1:
                live = jnp.int32(SHARED)
            keep = jnp.arange(SHARED, dtype=jnp.int32) < live
            slots_mine = jax.random.permutation(key_one, ST)[:SHARED].astype(jnp.int32)
            slots_theirs = jax.random.permutation(key_two, ST)[:SHARED].astype(jnp.int32)
            table = table.at[cluster_index, other].set(jnp.where(keep, slots_mine, -1))
            table = table.at[other, cluster_index].set(jnp.where(keep, slots_theirs, -1))
    return table


def set_ends(array, stream_key, least, largest):
    spot = [jax.random.randint(jax.random.fold_in(stream_key, axis), (), 0, length) for axis, length in enumerate(array.shape)]
    widest = array.shape.index(max(array.shape))
    beside = spot[:widest] + [(spot[widest] + 1) % array.shape[widest]] + spot[widest + 1:]
    return array.at[tuple(spot)].set(least).at[tuple(beside)].set(largest)


def block_levels(stream_key, extent, pieces, smallest, largest):
    gain = 1.0
    for dim, shards_of in pieces:
        steps = jax.random.uniform(jax.random.fold_in(jax.random.fold_in(stream_key, 6), dim), (shards_of,), jnp.float32, smallest / len(pieces), largest / len(pieces))
        gain = gain * jnp.repeat(jnp.exp(steps), extent[dim] // shards_of).reshape((-1,) + (1,) * (len(extent) - 1 - dim))
    return gain


def centred(stream_key, dims, width, most, pieces=(), held_as=jnp.bfloat16):
    loudness = block_levels(stream_key, dims, pieces, -0.22, 0.18) if pieces else 1.0
    array = jax.random.normal(stream_key, dims, jnp.float32) * width * loudness
    return jnp.minimum(jnp.maximum(array, -most), most).astype(held_as)


def setup_inputs(seed: int = 0) -> dict:
    splits = jax.random.split(jax.random.key(seed), 7)
    return {
        "visibilities": centred(splits[0], (CLUSTERS, 2, CHANNELS, SI, TS, BL), 2.0, 12.0, ((0, 4), (2, 8)), jnp.float32),
        "model": centred(splits[1], (CLUSTERS, 2, K, CHANNELS, SI, TS, BL), 1.0, 6.0, ((0, 4), (3, 8))),
        "flags": set_ends((jax.random.randint(splits[2], (CLUSTERS, CHANNELS, SI, TS, BL), 0, 8) < 1).astype(jnp.int32), jax.random.fold_in(splits[2], 1), 0, 1),
        "antennas": draw_antennas(jax.random.fold_in(splits[6], 71), 0),
        "correlation": draw_correlation(jax.random.fold_in(splits[6], 71), 0),
        "gains_init": centred(splits[5], (CLUSTERS, 2, K, CHANNELS, SI, ST), 0.8, 4.0, ((0, 4), (3, 8)), jnp.float32),
    }


def poly_basis(count):
    freq = jnp.arange(count, dtype=jnp.float32)
    xval = (2.0 * freq + 1.0) / count - 1.0
    return jnp.stack([jnp.ones_like(xval), xval, 1.5 * xval * xval - 0.5], axis=1)


def gram_inverse(basis):
    gram = jnp.dot(basis.T, basis, precision=lax.Precision.HIGHEST)
    cross_one = jnp.cross(gram[1], gram[2])
    cross_two = jnp.cross(gram[2], gram[0])
    cross_three = jnp.cross(gram[0], gram[1])
    determinant = jnp.sum(gram[0] * cross_one)
    return jnp.stack([cross_one, cross_two, cross_three], axis=1) / determinant


def model_terms(leading_receiver_jones, trailing_receiver_jones, vis, model, flag):
    model_re = model[0].astype(jnp.float32)
    model_im = model[1].astype(jnp.float32)
    weight = (1 - flag).astype(jnp.float32)
    prod_re = leading_receiver_jones[0] * trailing_receiver_jones[0] + leading_receiver_jones[1] * trailing_receiver_jones[1]
    prod_im = leading_receiver_jones[1] * trailing_receiver_jones[0] - leading_receiver_jones[0] * trailing_receiver_jones[1]
    pred_re = prod_re * model_re - prod_im * model_im
    pred_im = prod_re * model_im + prod_im * model_re
    res_re = weight * (vis[0] - jnp.sum(pred_re, axis=0))
    res_im = weight * (vis[1] - jnp.sum(pred_im, axis=0))
    return model_re, model_im, weight, pred_re, pred_im, res_re, res_im


def station_sides(leading_receiver_jones, trailing_receiver_jones, terms):
    model_re, model_im, weight, pred_re, pred_im, res_re, res_im = terms
    resid_re = res_re + weight * pred_re
    resid_im = res_im + weight * pred_im
    zed_re = trailing_receiver_jones[0] * model_re + trailing_receiver_jones[1] * model_im
    zed_im = trailing_receiver_jones[0] * model_im - trailing_receiver_jones[1] * model_re
    ups_re = leading_receiver_jones[0] * model_re - leading_receiver_jones[1] * model_im
    ups_im = leading_receiver_jones[0] * model_im + leading_receiver_jones[1] * model_re
    first_station_side = jnp.stack([
        jnp.sum(resid_re * zed_re + resid_im * zed_im, axis=-2),
        jnp.sum(resid_im * zed_re - resid_re * zed_im, axis=-2),
        jnp.sum(weight * (zed_re * zed_re + zed_im * zed_im), axis=-2)])
    second_station_side = jnp.stack([
        jnp.sum(resid_re * ups_re + resid_im * ups_im, axis=-2),
        jnp.sum(resid_re * ups_im - resid_im * ups_re, axis=-2),
        jnp.sum(weight * (ups_re * ups_re + ups_im * ups_im), axis=-2)])
    return first_station_side, second_station_side


def new_gains(summed_totals, target, penalty):
    return jnp.stack([(summed_totals[0] + penalty * target[0]) / (summed_totals[2] + penalty),
                      (summed_totals[1] + penalty * target[1]) / (summed_totals[2] + penalty)])


def reference(visibilities, model, flags, antennas, correlation, gains_init):
    high = lax.Precision.HIGHEST
    penalty = 2.0 * BL * TS / ST
    basis = poly_basis(CHANNELS)
    ginv = gram_inverse(basis)

    def fitted(values):
        partial_value = jnp.einsum('fn,akfsq->naksq', basis, values, precision=high)
        coef = jnp.einsum('mn,naksq->maksq', ginv, partial_value, precision=high)
        return jnp.einsum('fn,naksq->akfsq', basis, coef, precision=high)

    def segment_ids(side, index):
        moved = jnp.moveaxis(side, -1, 0)
        summed = jax.ops.segment_sum(moved, index, num_segments=ST)
        return jnp.moveaxis(summed, 0, -1)

    def update(cluster_index, final_jones_matrices, target):
        antenna_list = antennas[cluster_index]

        def one_channel(items):
            vis_c, model_c, flag_c, conjugate_gains, target_c = items
            leading_receiver_jones = conjugate_gains[:, :, :, antenna_list[0]][:, :, :, None, :]
            trailing_receiver_jones = conjugate_gains[:, :, :, antenna_list[1]][:, :, :, None, :]
            terms = model_terms(leading_receiver_jones, trailing_receiver_jones, vis_c, model_c, flag_c)
            first_station_side, second_station_side = station_sides(leading_receiver_jones, trailing_receiver_jones, terms)
            summed_totals = segment_ids(first_station_side, antenna_list[0]) + segment_ids(second_station_side, antenna_list[1])
            return new_gains(summed_totals, target_c, penalty)

        items = (jnp.moveaxis(visibilities[cluster_index], 1, 0), jnp.moveaxis(model[cluster_index], 2, 0),
                 flags[cluster_index], jnp.moveaxis(final_jones_matrices, 2, 0), jnp.moveaxis(target, 2, 0))
        return jnp.moveaxis(lax.map(one_channel, items), 0, 2)

    def residual(cluster_index, final_jones_matrices):
        antenna_list = antennas[cluster_index]

        def one_channel(items):
            vis_c, model_c, flag_c, conjugate_gains = items
            leading_receiver_jones = conjugate_gains[:, :, :, antenna_list[0]][:, :, :, None, :]
            trailing_receiver_jones = conjugate_gains[:, :, :, antenna_list[1]][:, :, :, None, :]
            terms = model_terms(leading_receiver_jones, trailing_receiver_jones, vis_c, model_c, flag_c)
            return jnp.stack([terms[5], terms[6]])

        items = (jnp.moveaxis(visibilities[cluster_index], 1, 0), jnp.moveaxis(model[cluster_index], 2, 0),
                 flags[cluster_index], jnp.moveaxis(final_jones_matrices, 2, 0))
        return jnp.moveaxis(lax.map(one_channel, items), 0, 1)

    def average(gains_all):
        shape = gains_all.shape
        flat = gains_all.reshape(CLUSTERS, -1, ST)
        iota = jnp.arange(ST, dtype=jnp.int32)
        result = []
        for cluster_index in range(CLUSTERS):
            total = flat[cluster_index]
            count = jnp.zeros((ST,), jnp.float32)
            for other in range(CLUSTERS):
                sel_mine = (correlation[cluster_index, other][:, None] == iota[None, :]).astype(jnp.float32)
                sel_theirs = (correlation[other, cluster_index][:, None] == iota[None, :]).astype(jnp.float32)
                received = jnp.einsum('js,rs->jr', sel_theirs, flat[other], precision=high)
                total = total + jnp.einsum('js,jr->rs', sel_mine, received, precision=high)
                count = count + jnp.sum(sel_mine, axis=0)
            result.append(total / (1.0 + count))
        return jnp.stack(result).reshape(shape)

    present_jones_matrices = gains_init
    dual = jnp.zeros_like(gains_init)
    agreed = jnp.stack([fitted(present_jones_matrices[c]) for c in range(CLUSTERS)])
    for step in range(ITERS):
        target = agreed - dual
        present_jones_matrices = jnp.stack([update(c, present_jones_matrices[c], target[c]) for c in range(CLUSTERS)])
        present_jones_matrices = average(present_jones_matrices)
        agreed = jnp.stack([fitted(present_jones_matrices[c] + dual[c]) for c in range(CLUSTERS)])
        dual = dual + present_jones_matrices - agreed
    residual_vis = jnp.stack([residual(c, present_jones_matrices[c]) for c in range(CLUSTERS)])
    return present_jones_matrices, agreed, residual_vis
```

```python
import functools

import jax
import jax.numpy as jnp
import numpy as np
from jax import lax
from jax.experimental import pallas as pl
from jax.experimental.pallas import tpu as pltpu
from jax.sharding import PartitionSpec as P

ITERS = 2
FITS = ITERS + 1
F32 = jnp.float32
BF16 = jnp.bfloat16


def gram_inverse(count):
    xval = (2.0 * np.arange(count) + 1.0) / count - 1.0
    basis = np.stack([np.ones_like(xval), xval, 1.5 * xval * xval - 0.5], axis=1)
    gram = basis.T @ basis
    cross = [np.cross(gram[1], gram[2]), np.cross(gram[2], gram[0]), np.cross(gram[0], gram[1])]
    return np.stack(cross, axis=1) / np.sum(gram[0] * cross[0])


def halves(values):
    high = values.astype(BF16)
    return high, (values - high.astype(F32)).astype(BF16)


def nt_dot(left, right):
    return lax.dot_general(left, right, (((1,), (1,)), ((), ())), preferred_element_type=F32)


def kernel(
    groups, chans, dirs, block, rho,
    mod, vis, flg, ant, corr, gin,
    jout, zout, rout,
    pick, both, tmat, ghl, gath, prods, dsum, whl, acc, jcur, dual, zcur,
    xsend, xall, ssend, zbuf, jsend, jrecv,
    fit_send, fit_recv, grp_send, grp_recv,
):
    grp = lax.axis_index("grp")
    me = lax.axis_index("chan")
    samples, si, lines = flg.shape
    slots = gin.shape[-1]
    steps = lines // block
    rows = xsend.shape[2]
    ginv = gram_inverse(chans)

    def chan_peer(d):
        return lax.rem(me + d, chans)

    def grp_peer(d):
        return lax.rem(grp + d, groups)

    barrier = pltpu.get_barrier_semaphore()

    def greet(d, carry):
        pl.semaphore_signal(barrier, inc=1, device_id={"chan": chan_peer(d)}, device_id_type=pl.DeviceIdType.MESH)
        return carry

    lax.fori_loop(1, chans, greet, 0)
    for d in range(1, groups):
        pl.semaphore_signal(barrier, inc=1, device_id={"grp": grp_peer(d)}, device_id_type=pl.DeviceIdType.MESH)

    jcur[:, :slots] = gin[0]
    jcur[:, slots:] = gin[1]
    dual[...] = jnp.zeros_like(dual)

    pl.semaphore_wait(barrier, chans - 1 + groups - 1)

    def spread(fit, phase, source, target):
        def send(d, carry):
            peer = chan_peer(d)
            pltpu.make_async_remote_copy(
                src_ref=source.at[fit, peer],
                dst_ref=target.at[fit, me],
                send_sem=fit_send.at[fit, phase],
                recv_sem=fit_recv.at[fit, phase],
                device_id={"chan": peer},
                device_id_type=pl.DeviceIdType.MESH,
            ).start()
            return carry

        lax.fori_loop(1, chans, send, 0)
        target[fit, me] = source[fit, me]

    def landed(fit, phase, source, target):
        pltpu.make_async_copy(source.at[fit, pl.ds(0, chans - 1)], source.at[fit, pl.ds(0, chans - 1)], fit_send.at[fit, phase]).wait()
        pltpu.make_async_copy(target.at[fit, pl.ds(0, chans - 1)], target.at[fit, pl.ds(0, chans - 1)], fit_recv.at[fit, phase]).wait()

    def fit_begin(fit):
        def fill(f, carry):
            part = pl.ds(pl.multiple_of(f * rows, rows), rows)
            xsend[fit, f] = jcur[part, :] + dual[part, :]
            return carry

        lax.fori_loop(0, chans, fill, 0)
        spread(fit, 0, xsend, xall)

    def basis_of(f):
        xval = (2 * f + 1).astype(F32) * (1.0 / chans) - 1.0
        return xval, 1.5 * xval * xval - 0.5

    def fit_middle(fit):
        landed(fit, 0, xsend, xall)

        def gather(f, sums):
            first, second = basis_of(f)
            value = xall[fit, f]
            return sums[0] + value, sums[1] + first * value, sums[2] + second * value

        zero = jnp.zeros(xall.shape[2:], F32)
        sums = lax.fori_loop(0, chans, gather, (zero, zero, zero))
        coef = [sum(float(ginv[n, m]) * sums[m] for m in range(3)) for n in range(3)]

        def expand(f, carry):
            first, second = basis_of(f)
            ssend[fit, f] = coef[0] + first * coef[1] + second * coef[2]
            return carry

        lax.fori_loop(0, chans, expand, 0)
        spread(fit, 1, ssend, zbuf)

    def fit_end(fit):
        landed(fit, 1, ssend, zbuf)

        def place(f, carry):
            zcur[pl.ds(pl.multiple_of(f * rows, rows), rows), :] = zbuf[fit, f]
            return carry

        lax.fori_loop(0, chans, place, 0)

    fit_begin(0)

    def build(step, carry):
        cols = pl.ds(pl.multiple_of(step * block, block), block)
        station = lax.broadcasted_iota(jnp.int32, (slots, block), 0)
        for side in range(2):
            hot = (station == ant[pl.ds(side, 1), cols]).astype(F32).astype(BF16)
            zero = jnp.zeros_like(hot)
            for part in range(2):
                for half in range(2):
                    base = 2 * slots * half
                    pick[side, part, base + part * slots : base + (part + 1) * slots, cols] = hot
                    base += (1 - part) * slots
                    pick[side, part, base : base + slots, cols] = zero
                both[side, part * slots : (part + 1) * slots, cols] = hot
        return carry

    lax.fori_loop(0, steps, build, 0)

    listed = corr.shape[-1]
    row = lax.broadcasted_iota(jnp.int32, (2 * slots, listed), 0)
    row = jnp.where(row >= slots, row - slots, row)
    block_row = lax.broadcasted_iota(jnp.int32, (2 * slots, 2 * slots), 0) >= slots
    block_col = lax.broadcasted_iota(jnp.int32, (2 * slots, 2 * slots), 1) >= slots
    count = jnp.zeros((1, 2 * slots), F32)
    for d in range(1, groups):
        other = grp_peer(d)
        mine = (row == corr[grp, pl.ds(other, 1), :]).astype(F32).astype(BF16)
        theirs = (row == corr[other, pl.ds(grp, 1), :]).astype(F32).astype(BF16)
        table = jnp.where(block_row == block_col, nt_dot(theirs, mine), 0.0).astype(BF16)
        tmat[d - 1, : 2 * slots, :] = table
        tmat[d - 1, 2 * slots :, :] = table
        count = count + nt_dot(jnp.ones((8, listed), BF16), mine)[:1]

    def split_gains():
        high, low = halves(jcur[...])
        ghl[:, : 2 * slots] = high
        ghl[:, 2 * slots :] = low

    def residual_of(cols):
        for side in range(2):
            for part in range(2):
                gath[side, part] = jnp.dot(ghl[...], pick[side, part, :, cols], preferred_element_type=F32)
        total = [[jnp.zeros((si, block), F32) for _ in range(2)] for _ in range(samples)]
        for k in range(dirs):
            at = slice(k * si, (k + 1) * si)
            are, aim, cre, cim = gath[0, 0, at], gath[0, 1, at], gath[1, 0, at], gath[1, 1, at]
            pre = are * cre + aim * cim
            pim = aim * cre - are * cim
            for t in range(samples):
                mre = mod[0, t, at, cols].astype(F32)
                mim = mod[1, t, at, cols].astype(F32)
                total[t][0] += pre * mre - pim * mim
                total[t][1] += pre * mim + pim * mre
        res, weights = [], []
        for t in range(samples):
            weight = (1 - flg[t, :, cols]).astype(F32)
            weights.append(weight)
            res.append([weight * (vis[part, t, :, cols] - total[t][part]) for part in range(2)])
        return res, weights

    def update_block(first, step, carry):
        cols = pl.ds(pl.multiple_of(step * block, block), block)
        res, weights = residual_of(cols)
        for k in range(dirs):
            at = slice(k * si, (k + 1) * si)
            low_at = slice((dirs + k) * si, (dirs + k + 1) * si)
            rre = rim = dd = 0.0
            for t in range(samples):
                mre = mod[0, t, at, cols].astype(F32)
                mim = mod[1, t, at, cols].astype(F32)
                rre += res[t][0] * mre + res[t][1] * mim
                rim += res[t][1] * mre - res[t][0] * mim
                if first:
                    dd += weights[t] * (mre * mre + mim * mim)
            if first:
                dsum[at, cols] = dd
            else:
                dd = dsum[at, cols]
            are, aim, cre, cim = gath[0, 0, at], gath[0, 1, at], gath[1, 0, at], gath[1, 1, at]
            sums = (
                rre * cre - rim * cim,
                rre * cim + rim * cre,
                dd * (cre * cre + cim * cim),
                rre * are + rim * aim,
                rre * aim - rim * are,
                dd * (are * are + aim * aim),
            )
            for i, value in enumerate(sums):
                high, low = halves(value)
                whl[i, at] = high
                whl[i, low_at] = low
        grad = den = None
        for side in range(2):
            for part in range(2):
                piece = nt_dot(whl[3 * side + part], pick[side, part, : 2 * slots, cols])
                grad = piece if grad is None else grad + piece
            piece = nt_dot(whl[3 * side + 2], both[side, :, cols])
            den = piece if den is None else den + piece
        acc[0] += grad
        acc[1] += den
        return carry

    def residual_block(step, carry):
        cols = pl.ds(pl.multiple_of(step * block, block), block)
        res, _ = residual_of(cols)
        for t in range(samples):
            for part in range(2):
                rout[part, t, :, cols] = res[t][part]
        return carry

    count_rows = dirs * si
    for it in range(ITERS):
        split_gains()
        acc[...] = jnp.zeros_like(acc)
        body = functools.partial(update_block, it == 0)
        middle = steps // 2
        lax.fori_loop(0, middle, body, 0)
        fit_middle(it)
        lax.fori_loop(middle, steps, body, 0)
        fit_end(it)
        present = jcur[...]
        if it > 0:
            dual[...] = dual[...] + present - zcur[...]
        den = acc[1, :count_rows] + acc[1, count_rows:]
        num = acc[0, :count_rows] + acc[0, count_rows:] + present * den
        updated = (num + rho * (zcur[...] - dual[...])) / (den + rho)
        jsend[it] = updated
        copies = []
        for d in range(1, groups):
            copy = pltpu.make_async_remote_copy(
                src_ref=jsend.at[it],
                dst_ref=jrecv.at[it, groups - d - 1],
                send_sem=grp_send.at[it, d - 1],
                recv_sem=grp_recv.at[it, groups - d - 1],
                device_id={"grp": grp_peer(d)},
                device_id_type=pl.DeviceIdType.MESH,
            )
            copy.start()
            copies.append(copy)
        total = updated
        for d in range(1, groups):
            pltpu.make_async_copy(jrecv.at[it, d - 1], jrecv.at[it, d - 1], grp_recv.at[it, d - 1]).wait()
            high, low = halves(jrecv[it, d - 1])
            total = total + jnp.dot(jnp.concatenate([high, low], axis=1), tmat[d - 1], preferred_element_type=F32)
        for copy in copies:
            copy.wait_send()
        jcur[...] = total / (1.0 + count)
        fit_begin(it + 1)

    split_gains()
    jout[0] = jcur[:, :slots]
    jout[1] = jcur[:, slots:]
    middle = steps // 2
    lax.fori_loop(0, middle, residual_block, 0)
    fit_middle(ITERS)
    lax.fori_loop(middle, steps, residual_block, 0)
    fit_end(ITERS)
    zout[0] = zcur[:, :slots]
    zout[1] = zcur[:, slots:]


def on_device(groups, chans, visibilities, model, flags, antennas, correlation, gains_init):
    _, _, dirs, _, si, samples, lines = model.shape
    slots = gains_init.shape[-1]
    count = dirs * si
    rho = 2.0 * lines * samples / slots
    block = min(256, lines)
    rows = count // chans
    mod = jnp.transpose(model[0, :, :, 0], (0, 3, 1, 2, 4)).reshape(2, samples, count, lines)
    vis = jnp.transpose(visibilities[0, :, 0], (0, 2, 1, 3))
    flg = jnp.transpose(flags[0, 0], (1, 0, 2))
    gin = gains_init.reshape(2, count, slots)
    vmem = pl.BlockSpec(memory_space=pltpu.VMEM)
    wide = 2 * slots
    jones, agreed, res = pl.pallas_call(
        functools.partial(kernel, groups, chans, dirs, block, rho),
        out_shape=(
            jax.ShapeDtypeStruct((2, count, slots), F32),
            jax.ShapeDtypeStruct((2, count, slots), F32),
            jax.ShapeDtypeStruct((2, samples, si, lines), F32),
        ),
        in_specs=[vmem] * 6,
        out_specs=(vmem, vmem, vmem),
        scratch_shapes=[
            pltpu.VMEM((2, 2, 2 * wide, lines), BF16),
            pltpu.VMEM((2, wide, lines), BF16),
            pltpu.VMEM((groups - 1, 2 * wide, wide), BF16),
            pltpu.VMEM((count, 2 * wide), BF16),
            pltpu.VMEM((2, 2, count, block), F32),
            pltpu.VMEM((2, count, block), F32),
            pltpu.VMEM((count, lines), F32),
            pltpu.VMEM((6, 2 * count, block), BF16),
            pltpu.VMEM((2, 2 * count, wide), F32),
            pltpu.VMEM((count, wide), F32),
            pltpu.VMEM((count, wide), F32),
            pltpu.VMEM((count, wide), F32),
            pltpu.VMEM((FITS, chans, rows, wide), F32),
            pltpu.VMEM((FITS, chans, rows, wide), F32),
            pltpu.VMEM((FITS, chans, rows, wide), F32),
            pltpu.VMEM((FITS, chans, rows, wide), F32),
            pltpu.VMEM((ITERS, count, wide), F32),
            pltpu.VMEM((ITERS, groups - 1, count, wide), F32),
            pltpu.SemaphoreType.DMA((FITS, 2)),
            pltpu.SemaphoreType.DMA((FITS, 2)),
            pltpu.SemaphoreType.DMA((ITERS, groups - 1)),
            pltpu.SemaphoreType.DMA((ITERS, groups - 1)),
        ],
        compiler_params=pltpu.CompilerParams(
            collective_id=0, has_side_effects=True, vmem_limit_bytes=48 * 1024 * 1024
        ),
    )(mod, vis, flg, antennas[0], correlation, gin)
    res = jnp.transpose(res, (0, 2, 1, 3))
    return (
        jones.reshape(gains_init.shape),
        agreed.reshape(gains_init.shape),
        res.reshape(visibilities.shape),
    )


def solution(mesh):
    return jax.shard_map(
        functools.partial(on_device, mesh.shape["grp"], mesh.shape["chan"]),
        mesh=mesh,
        in_specs=(
            P("grp", None, "chan", None, None, None),
            P("grp", None, None, "chan", None, None, None),
            P("grp", "chan", None, None, None),
            P("grp", None, None),
            P(),
            P("grp", None, None, "chan", None, None),
        ),
        out_specs=(
            P("grp", None, None, "chan", None, None),
            P("grp", None, None, "chan", None, None),
            P("grp", None, "chan", None, None, None),
        ),
        check_vma=False,
    )
```

```python
import functools

import jax
import jax.numpy as jnp
import numpy as np
from jax import lax
from jax.experimental import pallas as pl
from jax.experimental.pallas import tpu as pltpu
from jax.sharding import PartitionSpec as P

ITERS = 2
FITS = ITERS + 1
F32 = jnp.float32
BF16 = jnp.bfloat16
LANES = 128


def gram_inverse(count):
    xval = (2.0 * np.arange(count) + 1.0) / count - 1.0
    basis = np.stack([np.ones_like(xval), xval, 1.5 * xval * xval - 0.5], axis=1)
    gram = basis.T @ basis
    cross = [np.cross(gram[1], gram[2]), np.cross(gram[2], gram[0]), np.cross(gram[0], gram[1])]
    return np.stack(cross, axis=1) / np.sum(gram[0] * cross[0])


def halves(values):
    high = values.astype(BF16)
    return high, (values - high.astype(F32)).astype(BF16)


def nt_dot(left, right):
    return lax.dot_general(left, right, (((1,), (1,)), ((), ())), preferred_element_type=F32)


def kernel(
    groups, chans, dirs, block, rho,
    mod, vis, flg, ant, corr, gin,
    jout, zout, rout,
    pick, both, tmat, ghl, gath, prods, dsum, whl, acc, jcur, dual, zcur,
    xsend, xall, ssend, zbuf, jsend, jrecv,
    fit_send, fit_recv, grp_send, grp_recv,
):
    grp = lax.axis_index("grp")
    me = lax.axis_index("chan")
    samples, count_rows, lines = mod.shape[1:]
    si = count_rows // dirs
    per = block // LANES
    stride = lines // LANES * samples
    slots = gin.shape[-1]
    steps = lines // block
    rows = xsend.shape[2]
    ginv = gram_inverse(chans)

    def chan_peer(d):
        return lax.rem(me + d, chans)

    def grp_peer(d):
        return lax.rem(grp + d, groups)

    barrier = pltpu.get_barrier_semaphore()

    def greet(d, carry):
        pl.semaphore_signal(barrier, inc=1, device_id={"chan": chan_peer(d)}, device_id_type=pl.DeviceIdType.MESH)
        return carry

    lax.fori_loop(1, chans, greet, 0)
    for d in range(1, groups):
        pl.semaphore_signal(barrier, inc=1, device_id={"grp": grp_peer(d)}, device_id_type=pl.DeviceIdType.MESH)

    jcur[:, :slots] = gin[0]
    jcur[:, slots:] = gin[1]
    dual[...] = jnp.zeros_like(dual)

    pl.semaphore_wait(barrier, chans - 1 + groups - 1)

    owners = xsend.shape[1]
    least = (chans - owners) // 2
    owner = (me >= least) & (me < least + owners)
    mine_at = jnp.clip(me - least, 0, owners - 1)

    def send_to(source, target, fit, phase, peer):
        @pl.when(peer != me)
        def _():
            pltpu.make_async_remote_copy(
                src_ref=source,
                dst_ref=target,
                send_sem=fit_send.at[fit, phase],
                recv_sem=fit_recv.at[fit, phase],
                device_id={"chan": peer},
                device_id_type=pl.DeviceIdType.MESH,
            ).start()

    def took(ref, number, sem):
        part = ref.at[pl.ds(0, number)]
        pltpu.make_async_copy(part, part, sem).wait()

    def took_by_role(ref, sem):
        @pl.when(owner)
        def _():
            took(ref, owners - 1, sem)

        @pl.when(jnp.logical_not(owner))
        def _():
            took(ref, owners, sem)

    def fit_begin(fit):
        def fill(f, carry):
            part = pl.ds(pl.multiple_of(f * rows, rows), rows)
            xsend[fit, f] = jcur[part, :] + dual[part, :]
            return carry

        lax.fori_loop(0, owners, fill, 0)

        def send(n, carry):
            send_to(xsend.at[fit, n], xall.at[fit, me], fit, 0, least + n)
            return carry

        lax.fori_loop(0, owners, send, 0)

        @pl.when(owner)
        def _():
            xall[fit, me] = xsend[fit, mine_at]

    def basis_of(f):
        xval = (2 * f + 1).astype(F32) * (1.0 / chans) - 1.0
        return xval, 1.5 * xval * xval - 0.5

    def fit_middle(fit):
        took_by_role(xsend.at[fit], fit_send.at[fit, 0])

        @pl.when(owner)
        def _():
            took(xall.at[fit], chans - 1, fit_recv.at[fit, 0])

            def gather(f, sums):
                first, second = basis_of(f)
                value = xall[fit, f]
                return sums[0] + value, sums[1] + first * value, sums[2] + second * value

            zero = jnp.zeros(xall.shape[2:], F32)
            sums = lax.fori_loop(0, chans, gather, (zero, zero, zero))
            coef = [sum(float(ginv[n, m]) * sums[m] for m in range(3)) for n in range(3)]

            def expand(f, carry):
                first, second = basis_of(f)
                ssend[fit, f] = coef[0] + first * coef[1] + second * coef[2]
                return carry

            lax.fori_loop(0, chans, expand, 0)

            def send(f, carry):
                send_to(ssend.at[fit, f], zbuf.at[fit, mine_at], fit, 1, f)
                return carry

            lax.fori_loop(0, chans, send, 0)
            zbuf[fit, mine_at] = ssend[fit, me]

    def fit_end(fit):
        took_by_role(zbuf.at[fit], fit_recv.at[fit, 1])

        @pl.when(owner)
        def _():
            took(ssend.at[fit], chans - 1, fit_send.at[fit, 1])

        def place(f, carry):
            zcur[pl.ds(pl.multiple_of(f * rows, rows), rows), :] = zbuf[fit, f]
            return carry

        lax.fori_loop(0, owners, place, 0)

    fit_begin(0)

    def build(step, carry):
        cols = pl.ds(pl.multiple_of(step * block, block), block)
        station = lax.broadcasted_iota(jnp.int32, (slots, block), 0)
        for side in range(2):
            hot = (station == ant[pl.ds(side, 1), cols]).astype(F32).astype(BF16)
            zero = jnp.zeros_like(hot)
            for part in range(2):
                for half in range(2):
                    base = 2 * slots * half
                    pick[side, part, base + part * slots : base + (part + 1) * slots, cols] = hot
                    base += (1 - part) * slots
                    pick[side, part, base : base + slots, cols] = zero
                both[side, part * slots : (part + 1) * slots, cols] = hot
        return carry

    lax.fori_loop(0, steps, build, 0)

    listed = corr.shape[-1]
    wide = 2 * slots
    row = lax.broadcasted_iota(jnp.int32, (wide, 2 * listed), 0)
    place = lax.broadcasted_iota(jnp.int32, (wide, 2 * listed), 1)
    same = (row >= slots) == (place >= listed)
    row = jnp.where(row >= slots, row - slots, row)
    eye = lax.broadcasted_iota(jnp.int32, (2 * listed, 2 * listed), 0) == lax.broadcasted_iota(
        jnp.int32, (2 * listed, 2 * listed), 1
    )
    eye = eye.astype(F32).astype(BF16)
    for d in range(1, groups):
        mine = corr[grp, pl.ds(grp_peer(d), 1), :]
        hot = (same & (row == jnp.concatenate([mine, mine], axis=1))).astype(F32).astype(BF16)
        tmat[(d - 1) * 2 * listed : d * 2 * listed, :] = nt_dot(eye, hot).astype(BF16)
    count = jnp.dot(jnp.ones((8, tmat.shape[0]), BF16), tmat[...], preferred_element_type=F32)[:1]

    def lines_of(step, t):
        return [pl.ds((step * per + p) * samples + t, si, stride=stride) for p in range(per)]

    def read(ref, lead, step, t):
        return jnp.concatenate([ref[(*lead, part, slice(None))] for part in lines_of(step, t)], axis=1)

    def split_gains():
        high, low = halves(jcur[...])
        ghl[:, : 2 * slots] = high
        ghl[:, 2 * slots :] = low

    def residual_of(step, cols):
        for side in range(2):
            for part in range(2):
                gath[side, part] = jnp.dot(ghl[...], pick[side, part, :, cols], preferred_element_type=F32)
        total = [[jnp.zeros((si, block), F32) for _ in range(2)] for _ in range(samples)]
        for k in range(dirs):
            at = slice(k * si, (k + 1) * si)
            are, aim, cre, cim = gath[0, 0, at], gath[0, 1, at], gath[1, 0, at], gath[1, 1, at]
            pre = are * cre + aim * cim
            pim = aim * cre - are * cim
            for t in range(samples):
                mre = mod[0, t, at, cols].astype(F32)
                mim = mod[1, t, at, cols].astype(F32)
                total[t][0] += pre * mre - pim * mim
                total[t][1] += pre * mim + pim * mre
        res, weights = [], []
        for t in range(samples):
            weight = (1 - read(flg, (), step, t)).astype(F32)
            weights.append(weight)
            res.append([weight * (read(vis, (part,), step, t) - total[t][part]) for part in range(2)])
        return res, weights

    def update_block(first, step, carry):
        cols = pl.ds(pl.multiple_of(step * block, block), block)
        res, weights = residual_of(step, cols)
        for k in range(dirs):
            at = slice(k * si, (k + 1) * si)
            low_at = slice((dirs + k) * si, (dirs + k + 1) * si)
            rre = rim = dd = 0.0
            for t in range(samples):
                mre = mod[0, t, at, cols].astype(F32)
                mim = mod[1, t, at, cols].astype(F32)
                rre += res[t][0] * mre + res[t][1] * mim
                rim += res[t][1] * mre - res[t][0] * mim
                if first:
                    dd += weights[t] * (mre * mre + mim * mim)
            if first:
                dsum[at, cols] = dd
            else:
                dd = dsum[at, cols]
            are, aim, cre, cim = gath[0, 0, at], gath[0, 1, at], gath[1, 0, at], gath[1, 1, at]
            sums = (
                rre * cre - rim * cim,
                rre * cim + rim * cre,
                dd * (cre * cre + cim * cim),
                rre * are + rim * aim,
                rre * aim - rim * are,
                dd * (are * are + aim * aim),
            )
            for i, value in enumerate(sums):
                high, low = halves(value)
                whl[i, at] = high
                whl[i, low_at] = low
        grad = den = None
        for side in range(2):
            for part in range(2):
                piece = nt_dot(whl[3 * side + part], pick[side, part, : 2 * slots, cols])
                grad = piece if grad is None else grad + piece
            piece = nt_dot(whl[3 * side + 2], both[side, :, cols])
            den = piece if den is None else den + piece
        acc[0] += grad
        acc[1] += den
        return carry

    def residual_block(step, carry):
        cols = pl.ds(pl.multiple_of(step * block, block), block)
        res, _ = residual_of(step, cols)
        for t in range(samples):
            for part in range(2):
                for p, at in enumerate(lines_of(step, t)):
                    rout[part, at, :] = res[t][part][:, p * LANES : (p + 1) * LANES]
        return carry

    for it in range(ITERS):
        split_gains()
        acc[...] = jnp.zeros_like(acc)
        body = functools.partial(update_block, it == 0)
        middle = steps // 2
        lax.fori_loop(0, middle, body, 0)
        fit_middle(it)
        lax.fori_loop(middle, steps, body, 0)
        fit_end(it)
        present = jcur[...]
        if it > 0:
            dual[...] = dual[...] + present - zcur[...]
        den = acc[1, :count_rows] + acc[1, count_rows:]
        num = acc[0, :count_rows] + acc[0, count_rows:] + present * den
        updated = (num + rho * (zcur[...] - dual[...])) / (den + rho)
        high, low = halves(updated)
        shared = nt_dot(tmat[...], high) + nt_dot(tmat[...], low)
        copies = []
        for d in range(1, groups):
            jsend[it, d - 1] = shared[(d - 1) * 2 * listed : d * 2 * listed]
            copy = pltpu.make_async_remote_copy(
                src_ref=jsend.at[it, d - 1],
                dst_ref=jrecv.at[it, groups - d - 1],
                send_sem=grp_send.at[it, d - 1],
                recv_sem=grp_recv.at[it, groups - d - 1],
                device_id={"grp": grp_peer(d)},
                device_id_type=pl.DeviceIdType.MESH,
            )
            copy.start()
            copies.append(copy)
        for d in range(1, groups):
            pltpu.make_async_copy(jrecv.at[it, d - 1], jrecv.at[it, d - 1], grp_recv.at[it, d - 1]).wait()
        arrived = jnp.concatenate([jrecv[it, d] for d in range(groups - 1)], axis=0)
        high, low = halves(arrived.T)
        table = tmat[...]
        total = updated + jnp.dot(high, table, preferred_element_type=F32) + jnp.dot(low, table, preferred_element_type=F32)
        for copy in copies:
            copy.wait_send()
        jcur[...] = total / (1.0 + count)
        fit_begin(it + 1)

    split_gains()
    jout[0] = jcur[:, :slots]
    jout[1] = jcur[:, slots:]
    middle = steps // 2
    lax.fori_loop(0, middle, residual_block, 0)
    fit_middle(ITERS)
    lax.fori_loop(middle, steps, residual_block, 0)
    fit_end(ITERS)
    zout[0] = zcur[:, :slots]
    zout[1] = zcur[:, slots:]


def on_device(groups, chans, visibilities, model, flags, antennas, correlation, gains_init):
    _, _, dirs, _, si, samples, lines = model.shape
    slots = gains_init.shape[-1]
    count = dirs * si
    rho = 2.0 * lines * samples / slots
    block = min(256, lines)
    owners = max(chans // 2, 1)
    rows = count // owners
    mod = jnp.transpose(model[0, :, :, 0], (0, 3, 1, 2, 4)).reshape(2, samples, count, lines)
    tiles = lines // LANES

    def natural(values, *lead):
        split = values.reshape(*lead, si, samples, tiles, LANES)
        return jnp.swapaxes(split, -2, -3).reshape(*lead, si * tiles * samples, LANES)

    vis = natural(visibilities, 2)
    flg = natural(flags)
    gin = gains_init.reshape(2, count, slots)
    vmem = pl.BlockSpec(memory_space=pltpu.VMEM)
    wide = 2 * slots
    listed = correlation.shape[-1]
    jones, agreed, res = pl.pallas_call(
        functools.partial(kernel, groups, chans, dirs, block, rho),
        out_shape=(
            jax.ShapeDtypeStruct((2, count, slots), F32),
            jax.ShapeDtypeStruct((2, count, slots), F32),
            jax.ShapeDtypeStruct((2, si * tiles * samples, LANES), F32),
        ),
        in_specs=[vmem] * 6,
        out_specs=(vmem, vmem, vmem),
        scratch_shapes=[
            pltpu.VMEM((2, 2, 2 * wide, lines), BF16),
            pltpu.VMEM((2, wide, lines), BF16),
            pltpu.VMEM(((groups - 1) * 2 * listed, wide), BF16),
            pltpu.VMEM((count, 2 * wide), BF16),
            pltpu.VMEM((2, 2, count, block), F32),
            pltpu.VMEM((2, count, block), F32),
            pltpu.VMEM((count, lines), F32),
            pltpu.VMEM((6, 2 * count, block), BF16),
            pltpu.VMEM((2, 2 * count, wide), F32),
            pltpu.VMEM((count, wide), F32),
            pltpu.VMEM((count, wide), F32),
            pltpu.VMEM((count, wide), F32),
            pltpu.VMEM((FITS, owners, rows, wide), F32),
            pltpu.VMEM((FITS, chans, rows, wide), F32),
            pltpu.VMEM((FITS, chans, rows, wide), F32),
            pltpu.VMEM((FITS, owners, rows, wide), F32),
            pltpu.VMEM((ITERS, groups - 1, 2 * listed, count), F32),
            pltpu.VMEM((ITERS, groups - 1, 2 * listed, count), F32),
            pltpu.SemaphoreType.DMA((FITS, 2)),
            pltpu.SemaphoreType.DMA((FITS, 2)),
            pltpu.SemaphoreType.DMA((ITERS, groups - 1)),
            pltpu.SemaphoreType.DMA((ITERS, groups - 1)),
        ],
        compiler_params=pltpu.CompilerParams(
            collective_id=0, has_side_effects=True, vmem_limit_bytes=48 * 1024 * 1024
        ),
    )(mod, vis, flg, antennas[0], correlation, gin)
    res = jnp.swapaxes(res.reshape(2, si, tiles, samples, LANES), -2, -3)
    return (
        jones.reshape(gains_init.shape),
        agreed.reshape(gains_init.shape),
        res.reshape(visibilities.shape),
    )


def solution(mesh):
    return jax.shard_map(
        functools.partial(on_device, mesh.shape["grp"], mesh.shape["chan"]),
        mesh=mesh,
        in_specs=(
            P("grp", None, "chan", None, None, None),
            P("grp", None, None, "chan", None, None, None),
            P("grp", "chan", None, None, None),
            P("grp", None, None),
            P(),
            P("grp", None, None, "chan", None, None),
        ),
        out_specs=(
            P("grp", None, None, "chan", None, None),
            P("grp", None, None, "chan", None, None),
            P("grp", None, "chan", None, None, None),
        ),
        check_vma=False,
    )
```
